32 devices in a mesh: section: 16 (over z, y, core), tensor: 2 (over x).
Axes of the slice: x: 2, y: 2, z: 4, core: 2. Of those that a mesh axis runs over, the one named last changes fastest.
Arguments:
- saved: bfloat16 [16, 16, 64, 8192], P('section', None, 'tensor'), may hold values from -6 to 6
- offsets: int32 [16, 16], P('section'), may hold values from 0 to 15, as said below
Outputs:
- restored: float32 [16, 16, 64, 8192], P('section', None, None, 'tensor')
- block_sums: float32 [16, 16, 8192], P('section', None, 'tensor')
The draws below stay inside these ranges and needn't reach their ends.
Inputs may be any that keep to these rules, and one draw needn't show every extreme that they name: Each row of offsets is a permutation of 0 to 15.
All inputs are finite; a program needn't handle non-finite values.
Results may differ from the reference program's by a relative error of at most 0.0003.
Values may be sent and summed in bfloat16 or wider, within the bound.
A program may use at most 128 MiB of HBM per device.

```python
import jax
import jax.numpy as jnp

D = 8192
R = 64
SLOTS = 16
N_SECTION = 16


def draw_offsets(key, part):
    row_keys = jax.random.split(jax.random.fold_in(key, 17), N_SECTION)
    rows = jax.vmap(lambda k: jax.random.permutation(k, N_SECTION))(row_keys)
    return rows.astype(jnp.int32)


def shard_levels(stream_key, dims, cuts, least, largest):
    def one(dim, parts):
        draws = jax.random.uniform(jax.random.fold_in(jax.random.fold_in(stream_key, 6), dim), (parts,), jnp.float32, least / len(cuts), largest / len(cuts))
        return jnp.repeat(jnp.exp(draws), dims[dim] // parts).reshape((-1,) + (1,) * (len(dims) - dim - 1))

    factor_of = one(*cuts[0])
    for cut in cuts[1:]:
        factor_of = factor_of * one(*cut)
    return factor_of


def gaussian(stream_key, dims, width, limit, cuts=(), kind=jnp.bfloat16):
    loudness = shard_levels(stream_key, dims, cuts, -0.22, 0.18) if cuts else 1.0
    entries = jax.random.normal(stream_key, dims, jnp.float32) * width * loudness
    return jnp.minimum(jnp.maximum(entries, -limit), limit).astype(kind)


def setup_inputs(seed: int = 0) -> dict:
    keys = jax.random.split(jax.random.key(seed), 3)
    return {
        "saved": gaussian(keys[0], (N_SECTION, SLOTS, R, D), 1.0, 6.0, ((0, 16), (2, 2))),
        "offsets": draw_offsets(jax.random.fold_in(keys[2], 71), 0),
    }


def reference(saved, offsets):
    sections = jnp.arange(N_SECTION, dtype=jnp.int32)
    relative = ((sections[:, None] - sections[None, :]) % N_SECTION).astype(jnp.int32)
    inverse = jnp.argsort(offsets, axis=1).astype(jnp.int32)
    sources = jnp.broadcast_to(sections[None, :], (N_SECTION, N_SECTION)).astype(jnp.int32)
    chosen = inverse[sources, relative]
    blocks = saved[sources, chosen]
    restored = blocks.astype(jnp.float32)
    block_sums = jnp.sum(restored, axis=2)
    return restored, block_sums
```

```python
import jax
import jax.numpy as jnp
from jax import lax
from jax.experimental import pallas as pl
from jax.experimental.pallas import tpu as pltpu
from jax.sharding import PartitionSpec as P

MESH = pl.DeviceIdType.MESH


def power_of_two(count):
    return count & (count - 1) == 0


def partner(index, step, count):
    if not power_of_two(count):
        return (index + step) % count
    other = index
    bit = 1
    while bit < count:
        if step & bit:
            other = other + bit * (1 - 2 * ((index // bit) % 2))
        bit *= 2
    return other


def late_steps(n):
    if n < 8 or not power_of_two(n):
        return []
    return list(range(3 * n // 4, n, 2))


def is_late(s, n):
    quarter = s // (n // 4)
    return ((quarter == 1) | (quarter == 2)) & (s % 2 == 0)


def send_order(n, m):
    late = late_steps(n)
    far_steps = [k for k in range(n // 2, n) if k not in late] + late
    far = [(k, e) for k in far_steps for e in range(m)]
    near = [(k, e) for k in range(n // 2 - 1, -1, -1) for e in range(m)]
    mixed = []
    for i in range(max(len(far), len(near))):
        mixed += far[i : i + 1] + near[i : i + 1]
    return mixed


def exchange(n, m, offsets, saved, arrived, kept, held, out_box, load_sem, send_sem, recv_sem, own_sem):
    s = lax.axis_index("section")
    x = lax.axis_index("tensor")
    rows = saved.shape[1]
    cols = saved.shape[2] // m
    late = late_steps(n)
    early = [k for k in range(n) if k not in late]
    load = pltpu.make_async_copy(saved, held, load_sem)
    load.start()

    barrier = pltpu.get_barrier_semaphore()

    def greet(i, carry):
        j = i + 1
        pl.semaphore_signal(
            barrier,
            inc=1,
            device_id=((s + j // m) % n, (x + j % m) % m),
            device_id_type=MESH,
        )
        return carry

    lax.fori_loop(0, n * m - 1, greet, 0)
    load.wait()

    def box(k, e):
        if k in late:
            return kept.at[late.index(k) * m + e]
        return out_box.at[early.index(k) * m + e]

    def send(k, e):
        t = partner(s, k, n)
        d = partner(x, e, m)
        dst = arrived.at[s, pl.ds(x * rows, rows), :]
        if k == 0 and e == 0:
            return pltpu.make_async_copy(box(k, e), dst, own_sem)
        return pltpu.make_async_remote_copy(
            src_ref=box(k, e),
            dst_ref=dst,
            send_sem=send_sem.at[k * m + e],
            recv_sem=recv_sem.at[k * m + e],
            device_id=(t, d),
            device_id_type=MESH,
        )

    def fill(k, e):
        t = partner(s, k, n)
        d = partner(x, e, m)
        wanted = (t - s + n) % n
        slot = jnp.int32(0)
        for j in range(n):
            slot = jnp.where(offsets[0, j] == wanted, jnp.int32(j), slot)
        step = min(cols, 512)
        to = box(k, e)

        def move(i, carry):
            src = pl.ds(pl.multiple_of(d * cols + i * step, step), step)
            dst = pl.ds(pl.multiple_of(i * step, step), step)
            to[:, dst] = held[slot, :, src]
            return carry

        lax.fori_loop(0, cols // step, move, 0)

    def start(k, e):
        copy = send(k, e)
        if k in late:
            pl.when(jnp.logical_not(is_late(s, n)))(copy.start)
        else:
            copy.start()
        copies.append((k, copy))

    copies = []
    waiting = None
    for k, e in send_order(n, m):
        fill(k, e)
        if waiting is not None:
            if not copies:
                pl.semaphore_wait(barrier, n * m - 1)
            start(*waiting)
        waiting = (k, e)
    start(*waiting)
    for k, copy in copies:
        if k not in late:
            copy.wait()

    if late:

        @pl.when(jnp.logical_not(is_late(s, n)))
        def _():
            for k, copy in copies:
                if k in late:
                    copy.wait()


def exchange_late(n, m, kept, sums, arrived, send_sem, recv_sem):
    s = lax.axis_index("section")
    x = lax.axis_index("tensor")
    rows = kept.shape[1]
    late = late_steps(n)
    pairs = [(k, e) for k in late for e in range(m)]
    barrier = pltpu.get_barrier_semaphore()

    @pl.when(is_late(s, n))
    def _():
        for k, e in pairs:
            pl.semaphore_signal(
                barrier,
                inc=1,
                device_id=(partner(s, k, n), partner(x, e, m)),
                device_id_type=MESH,
            )
        pl.semaphore_wait(barrier, len(pairs))
        copies = []
        for i, (k, e) in enumerate(pairs):
            copy = pltpu.make_async_remote_copy(
                src_ref=kept.at[i],
                dst_ref=arrived.at[late.index(k), pl.ds(x * rows, rows), :],
                send_sem=send_sem.at[i],
                recv_sem=recv_sem.at[i],
                device_id=(partner(s, k, n), partner(x, e, m)),
                device_id_type=MESH,
            )
            copy.start()
            copies.append(copy)
        for copy in copies:
            copy.wait()


def widen_block(arrived, i, restored, sums, at, stage, sem):
    _, rows, cols = arrived.shape
    wide = min(cols, 512)
    for c in range(0, cols, wide):
        here = pl.ds(c, wide)
        total = None
        for r in range(0, rows, 16):
            band = pl.ds(r, min(16, rows - r))
            part = arrived[i, band, here].astype(jnp.float32)
            stage[band, here] = part
            total = part if total is None else total + part
        sums[pl.ds(at, 1), here] = jnp.sum(total, axis=0, keepdims=True)
    copy = pltpu.make_async_copy(stage, restored.at[at], sem)
    copy.start()
    return copy


def widen(n, arrived, restored, sums, stage, table, stage_sem):
    s = lax.axis_index("section")
    late = late_steps(n)
    depth = stage.shape[0] - len(late)
    copies = []
    for k in range(n):
        if k in late:
            continue
        slot = len(copies) % depth
        if len(copies) >= depth:
            copies[len(copies) - depth].wait()
        i = partner(s, k, n)
        copies.append(
            widen_block(arrived, i, restored, table, i, stage.at[slot], stage_sem.at[slot])
        )
    if late:

        @pl.when(jnp.logical_not(is_late(s, n)))
        def _():
            rest = []
            for j, k in enumerate(late):
                i = partner(s, k, n)
                slot = depth + j
                rest.append(
                    widen_block(arrived, i, restored, table, i, stage.at[slot], stage_sem.at[slot])
                )
            for copy in rest:
                copy.wait()

    sums[...] = table[pl.ds(0, n), :]
    for copy in copies[-depth:]:
        copy.wait()


def widen_late(n, arrived, given, sums, restored, sums_out, stage, table, stage_sem, table_sem):
    s = lax.axis_index("section")
    late = late_steps(n)
    table[pl.ds(0, n), :] = sums[...]

    @pl.when(is_late(s, n))
    def _():
        rest = []
        for j, k in enumerate(late):
            i = partner(s, k, n)
            rest.append(
                widen_block(arrived, j, restored, table, i, stage.at[j], stage_sem.at[j])
            )
        for copy in rest:
            copy.wait()

    copy = pltpu.make_async_copy(table.at[pl.ds(0, n), :], sums_out, table_sem)
    copy.start()
    copy.wait()


def body(n, m, saved, offsets):
    _, slots, rows, width = saved.shape
    cols = width // m
    late = len(late_steps(n))
    arrived, kept = pl.pallas_call(
        lambda *refs: exchange(n, m, *refs),
        out_shape=[
            jax.ShapeDtypeStruct((slots, rows * m, cols), saved.dtype),
            jax.ShapeDtypeStruct((max(late * m, 1), rows, cols), saved.dtype),
        ],
        in_specs=[
            pl.BlockSpec(memory_space=pltpu.SMEM),
            pl.BlockSpec(memory_space=pltpu.HBM),
        ],
        out_specs=[
            pl.BlockSpec(memory_space=pl.ANY),
            pl.BlockSpec(memory_space=pltpu.VMEM),
        ],
        scratch_shapes=[
            pltpu.VMEM((slots, rows, width), saved.dtype),
            pltpu.VMEM(((slots - late) * m, rows, cols), saved.dtype),
            pltpu.SemaphoreType.DMA,
            pltpu.SemaphoreType.DMA((n * m,)),
            pltpu.SemaphoreType.DMA((n * m,)),
            pltpu.SemaphoreType.DMA,
        ],
        compiler_params=pltpu.CompilerParams(
            collective_id=0, has_side_effects=True, vmem_limit_bytes=20 * 2**20
        ),
        name="exchange",
    )(offsets, pltpu.with_memory_space_constraint(saved[0], pltpu.HBM))
    blocks, height = arrived.shape[:2]
    restored, block_sums = pl.pallas_call(
        lambda *refs: widen(n, *refs),
        out_shape=[
            jax.ShapeDtypeStruct(arrived.shape, jnp.float32),
            jax.ShapeDtypeStruct((blocks, cols), jnp.float32),
        ],
        in_specs=[pl.BlockSpec(memory_space=pltpu.VMEM)],
        out_specs=[
            pl.BlockSpec(memory_space=pl.ANY),
            pl.BlockSpec(memory_space=pltpu.VMEM),
        ],
        scratch_shapes=[
            pltpu.VMEM((6 + late, height, cols), jnp.float32),
            pltpu.VMEM((blocks + 8, cols), jnp.float32),
            pltpu.SemaphoreType.DMA((6 + late,)),
        ],
        compiler_params=pltpu.CompilerParams(vmem_limit_bytes=20 * 2**20),
        name="widen",
    )(arrived)
    if late:
        arrived = pl.pallas_call(
            lambda *refs: exchange_late(n, m, *refs),
            out_shape=jax.ShapeDtypeStruct((late, rows * m, cols), saved.dtype),
            in_specs=[
                pl.BlockSpec(memory_space=pltpu.VMEM),
                pl.BlockSpec(memory_space=pl.ANY),
            ],
            out_specs=pl.BlockSpec(memory_space=pl.ANY),
            scratch_shapes=[
                pltpu.SemaphoreType.DMA((late * m,)),
                pltpu.SemaphoreType.DMA((late * m,)),
            ],
            compiler_params=pltpu.CompilerParams(
                collective_id=1, has_side_effects=True, vmem_limit_bytes=8 * 2**20
            ),
            name="exchange_late",
        )(kept, block_sums)
        restored, block_sums = pl.pallas_call(
            lambda *refs: widen_late(n, *refs),
            out_shape=[
                jax.ShapeDtypeStruct(restored.shape, jnp.float32),
                jax.ShapeDtypeStruct(block_sums.shape, jnp.float32),
            ],
            in_specs=[
                pl.BlockSpec(memory_space=pltpu.VMEM),
                pl.BlockSpec(memory_space=pl.ANY),
                pl.BlockSpec(memory_space=pltpu.VMEM),
            ],
            out_specs=[
                pl.BlockSpec(memory_space=pl.ANY),
                pl.BlockSpec(memory_space=pl.ANY),
            ],
            scratch_shapes=[
                pltpu.VMEM((late, height, cols), jnp.float32),
                pltpu.VMEM((blocks + 8, cols), jnp.float32),
                pltpu.SemaphoreType.DMA((late,)),
                pltpu.SemaphoreType.DMA,
            ],
            input_output_aliases={1: 0},
            compiler_params=pltpu.CompilerParams(vmem_limit_bytes=20 * 2**20),
            name="widen_late",
        )(arrived, restored, block_sums)
    return (restored[None], block_sums[None])


def solution(mesh):
    n = mesh.shape["section"]
    m = mesh.shape["tensor"]
    return jax.shard_map(
        lambda saved, offsets: body(n, m, saved, offsets),
        mesh=mesh,
        in_specs=(P("section", None, "tensor", None), P("section", None)),
        out_specs=(P("section", None, None, "tensor"), P("section", None, "tensor")),
        check_vma=False,
    )
```

```python
import jax
import jax.numpy as jnp
from jax import lax
from jax.experimental import pallas as pl
from jax.experimental.pallas import tpu as pltpu
from jax.sharding import PartitionSpec as P

MESH = pl.DeviceIdType.MESH


def power_of_two(count):
    return count & (count - 1) == 0


def partner(index, step, count):
    if not power_of_two(count):
        return (index + step) % count
    other = index
    bit = 1
    while bit < count:
        if step & bit:
            other = other + bit * (1 - 2 * ((index // bit) % 2))
        bit *= 2
    return other


def late_steps(n):
    if n < 8 or not power_of_two(n):
        return []
    return list(range(3 * n // 4, n, 2))


def is_inner(s, n):
    quarter = s // (n // 4)
    return (quarter == 1) | (quarter == 2)


def is_late(s, n):
    return is_inner(s, n) & (s % 2 == 0)


def early_step(n):
    return 3 * n // 4 + 1


def send_order(n, m):
    late = late_steps(n)
    far_steps = [k for k in range(n // 2, n) if k not in late] + late
    far = [(k, e) for k in far_steps for e in range(m)]
    near = [(k, e) for k in range(n // 2 - 1, -1, -1) for e in range(m)]
    mixed = []
    for i in range(max(len(far), len(near))):
        mixed += far[i : i + 1] + near[i : i + 1]
    return mixed


def parts_of(rows):
    return 2 if rows % 32 == 0 else 1


def signal(barrier, t, d):
    pl.semaphore_signal(barrier, inc=1, device_id=(t, d), device_id_type=MESH)


def greet_outer(barrier, n, m, first, s, x):
    half = n // 2

    def greet(j, carry):
        place = (s + j // m) % half
        t = jnp.where(place < n // 4, place, place + half)
        signal(barrier, t, (x + j % m) % m)
        return carry

    lax.fori_loop(first, half * m, greet, 0)


def greet_all(barrier, n, m, s, x):
    def greet(j, carry):
        signal(barrier, (s + j // m) % n, (x + j % m) % m)
        return carry

    lax.fori_loop(1, n * m, greet, 0)


def exchange(
    n, m, offsets, saved, arrived, kept, table, rest, out_box,
    table_sem, load_sem, send_sem, recv_sem, own_sem, part_sem, *pieces,
):
    s = lax.axis_index("section")
    x = lax.axis_index("tensor")
    rows = saved.shape[1]
    cols = saved.shape[2] // m
    parts = len(pieces)
    part = rows // parts
    late = late_steps(n)
    staged = bool(late)
    first = early_step(n) if staged else n // 2
    barrier = pltpu.get_barrier_semaphore()
    inner = is_inner(s, n) if staged else None

    tabled = pltpu.make_async_copy(offsets, table, table_sem)
    tabled.start()
    own = pl.ds(pl.multiple_of(x * cols, cols), cols)
    loads = [
        pltpu.make_async_copy(saved.at[:, pl.ds(h * part, part), own], piece, load_sem.at[h])
        for h, piece in enumerate(pieces)
    ]
    for e in range(1, m):
        d = partner(x, e, m)
        those = pl.ds(pl.multiple_of(d * cols, cols), cols)
        loads.append(
            pltpu.make_async_copy(saved.at[:, :, those], rest.at[e - 1], load_sem.at[parts - 1 + e])
        )
    for load in loads:
        load.start()

    if staged:

        @pl.when(inner)
        def _():
            signal(barrier, partner(s, first, n), x)

        @pl.when(jnp.logical_not(inner))
        def _():
            greet_outer(barrier, n, m, 1, jnp.where(s < n // 4, s, s - n // 2), x)

    else:
        greet_all(barrier, n, m, s, x)

    early = [k for k in range(n) if k not in late]

    def box(k, e):
        if k in late:
            return kept.at[late.index(k) * m + e]
        return out_box.at[early.index(k) * m + e]

    def slot_of(k):
        wanted = (partner(s, k, n) - s + n) % n
        slot = jnp.int32(0)
        for j in range(n):
            slot = jnp.where(table[0, j] == wanted, jnp.int32(j), slot)
        return slot

    def fill(held, slot, to):
        step = min(cols, 512)

        def move(i, carry):
            here = pl.ds(pl.multiple_of(i * step, step), step)
            to[:, here] = held[slot, :, here]
            return carry

        lax.fori_loop(0, cols // step, move, 0)

    def fill_block(k, e):
        slot = slot_of(k)
        to = box(k, e)
        if e == 0:
            for h, piece in enumerate(pieces):
                fill(piece, slot, to.at[pl.ds(h * part, part), :])
        else:
            fill(rest.at[e - 1], slot, to)

    def send(k, e):
        dst = arrived.at[s, pl.ds(x * rows, rows), :]
        if k == 0 and e == 0:
            return pltpu.make_async_copy(box(k, e), dst, own_sem)
        return pltpu.make_async_remote_copy(
            src_ref=box(k, e),
            dst_ref=dst,
            send_sem=send_sem.at[k * m + e],
            recv_sem=recv_sem.at[k * m + e],
            device_id=(partner(s, k, n), partner(x, e, m)),
            device_id_type=MESH,
        )

    def send_part(h):
        return pltpu.make_async_remote_copy(
            src_ref=box(first, 0).at[pl.ds(h * part, part), :],
            dst_ref=arrived.at[s, pl.ds(x * rows + h * part, part), :],
            send_sem=part_sem.at[h],
            recv_sem=part_sem.at[parts + h],
            device_id=(partner(s, first, n), x),
            device_id_type=MESH,
        )

    firsts = [send_part(h) for h in range(parts)]
    tabled.wait()
    slot = slot_of(first)
    for h in range(parts):
        loads[h].wait()
        fill(pieces[h], slot, box(first, 0).at[pl.ds(h * part, part), :])
        if h > 0:
            firsts[h].start()
        elif staged:

            @pl.when(inner)
            def _():
                pl.semaphore_wait(barrier, 1)
                firsts[0].start()
                greet_outer(barrier, n, m, 0, 0, 0)

            @pl.when(jnp.logical_not(inner))
            def _():
                pl.semaphore_wait(barrier, n * m - 1)
                signal(barrier, partner(s, n // 4, n), x)
                firsts[0].start()

        else:
            pl.semaphore_wait(barrier, n * m - 1)
            firsts[0].start()
    for load in loads[parts:]:
        load.wait()

    def start(k, e):
        copy = send(k, e)
        if k in late:
            pl.when(jnp.logical_not(is_late(s, n)))(copy.start)
        else:
            copy.start()
        copies.append((k, copy))

    copies = []
    waiting = None
    for k, e in send_order(n, m):
        if k == first and e == 0:
            continue
        fill_block(k, e)
        if waiting is not None:
            if staged and not copies:

                @pl.when(inner)
                def _():
                    pl.semaphore_wait(barrier, 1)

            start(*waiting)
        waiting = (k, e)
    start(*waiting)
    for copy in firsts:
        copy.wait()
    for k, copy in copies:
        if k not in late:
            copy.wait()

    if late:

        @pl.when(jnp.logical_not(is_late(s, n)))
        def _():
            for k, copy in copies:
                if k in late:
                    copy.wait()


def exchange_late(n, m, kept, sums, arrived, send_sem, recv_sem):
    s = lax.axis_index("section")
    x = lax.axis_index("tensor")
    rows = kept.shape[1]
    late = late_steps(n)
    pairs = [(k, e) for k in late for e in range(m)]
    barrier = pltpu.get_barrier_semaphore()

    @pl.when(is_late(s, n))
    def _():
        for k, e in pairs:
            pl.semaphore_signal(
                barrier,
                inc=1,
                device_id=(partner(s, k, n), partner(x, e, m)),
                device_id_type=MESH,
            )
        pl.semaphore_wait(barrier, len(pairs))
        copies = []
        for i, (k, e) in enumerate(pairs):
            copy = pltpu.make_async_remote_copy(
                src_ref=kept.at[i],
                dst_ref=arrived.at[late.index(k), pl.ds(x * rows, rows), :],
                send_sem=send_sem.at[i],
                recv_sem=recv_sem.at[i],
                device_id=(partner(s, k, n), partner(x, e, m)),
                device_id_type=MESH,
            )
            copy.start()
            copies.append(copy)
        for copy in copies:
            copy.wait()


def widen_block(arrived, i, restored, sums, at, stage, sem):
    _, rows, cols = arrived.shape
    wide = min(cols, 512)
    for c in range(0, cols, wide):
        here = pl.ds(c, wide)
        total = None
        for r in range(0, rows, 16):
            band = pl.ds(r, min(16, rows - r))
            part = arrived[i, band, here].astype(jnp.float32)
            stage[band, here] = part
            total = part if total is None else total + part
        sums[pl.ds(at, 1), here] = jnp.sum(total, axis=0, keepdims=True)
    copy = pltpu.make_async_copy(stage, restored.at[at], sem)
    copy.start()
    return copy


def widen(n, arrived, restored, sums, stage, table, stage_sem):
    s = lax.axis_index("section")
    late = late_steps(n)
    depth = stage.shape[0] - len(late)
    copies = []
    for k in range(n):
        if k in late:
            continue
        slot = len(copies) % depth
        if len(copies) >= depth:
            copies[len(copies) - depth].wait()
        i = partner(s, k, n)
        copies.append(
            widen_block(arrived, i, restored, table, i, stage.at[slot], stage_sem.at[slot])
        )
    if late:

        @pl.when(jnp.logical_not(is_late(s, n)))
        def _():
            rest = []
            for j, k in enumerate(late):
                i = partner(s, k, n)
                slot = depth + j
                rest.append(
                    widen_block(arrived, i, restored, table, i, stage.at[slot], stage_sem.at[slot])
                )
            for copy in rest:
                copy.wait()

    sums[...] = table[pl.ds(0, n), :]
    for copy in copies[-depth:]:
        copy.wait()


def widen_late(n, arrived, given, sums, restored, sums_out, stage, table, stage_sem, table_sem):
    s = lax.axis_index("section")
    late = late_steps(n)
    table[pl.ds(0, n), :] = sums[...]

    @pl.when(is_late(s, n))
    def _():
        rest = []
        for j, k in enumerate(late):
            i = partner(s, k, n)
            rest.append(
                widen_block(arrived, j, restored, table, i, stage.at[j], stage_sem.at[j])
            )
        for copy in rest:
            copy.wait()

    copy = pltpu.make_async_copy(table.at[pl.ds(0, n), :], sums_out, table_sem)
    copy.start()
    copy.wait()


def body(n, m, saved, offsets):
    _, slots, rows, width = saved.shape
    cols = width // m
    late = len(late_steps(n))
    parts = parts_of(rows)
    arrived, kept = pl.pallas_call(
        lambda *refs: exchange(n, m, *refs),
        out_shape=[
            jax.ShapeDtypeStruct((slots, rows * m, cols), saved.dtype),
            jax.ShapeDtypeStruct((max(late * m, 1), rows, cols), saved.dtype),
        ],
        in_specs=[
            pl.BlockSpec(memory_space=pltpu.HBM),
            pl.BlockSpec(memory_space=pltpu.HBM),
        ],
        out_specs=[
            pl.BlockSpec(memory_space=pl.ANY),
            pl.BlockSpec(memory_space=pltpu.VMEM),
        ],
        scratch_shapes=[
            pltpu.SMEM(offsets.shape, offsets.dtype),
            pltpu.VMEM((max(m - 1, 1), slots, rows, cols), saved.dtype),
            pltpu.VMEM(((slots - late) * m, rows, cols), saved.dtype),
            pltpu.SemaphoreType.DMA,
            pltpu.SemaphoreType.DMA((parts + m - 1,)),
            pltpu.SemaphoreType.DMA((n * m,)),
            pltpu.SemaphoreType.DMA((n * m,)),
            pltpu.SemaphoreType.DMA,
            pltpu.SemaphoreType.DMA((2 * parts,)),
        ]
        + [pltpu.VMEM((slots, rows // parts, cols), saved.dtype)] * parts,
        compiler_params=pltpu.CompilerParams(
            collective_id=0, has_side_effects=True, vmem_limit_bytes=20 * 2**20
        ),
        name="exchange",
    )(
        pltpu.with_memory_space_constraint(offsets, pltpu.HBM),
        pltpu.with_memory_space_constraint(saved[0], pltpu.HBM),
    )
    blocks, height = arrived.shape[:2]
    restored, block_sums = pl.pallas_call(
        lambda *refs: widen(n, *refs),
        out_shape=[
            jax.ShapeDtypeStruct(arrived.shape, jnp.float32),
            jax.ShapeDtypeStruct((blocks, cols), jnp.float32),
        ],
        in_specs=[pl.BlockSpec(memory_space=pltpu.VMEM)],
        out_specs=[
            pl.BlockSpec(memory_space=pl.ANY),
            pl.BlockSpec(memory_space=pltpu.VMEM),
        ],
        scratch_shapes=[
            pltpu.VMEM((6 + late, height, cols), jnp.float32),
            pltpu.VMEM((blocks + 8, cols), jnp.float32),
            pltpu.SemaphoreType.DMA((6 + late,)),
        ],
        compiler_params=pltpu.CompilerParams(vmem_limit_bytes=20 * 2**20),
        name="widen",
    )(arrived)
    if late:
        arrived = pl.pallas_call(
            lambda *refs: exchange_late(n, m, *refs),
            out_shape=jax.ShapeDtypeStruct((late, rows * m, cols), saved.dtype),
            in_specs=[
                pl.BlockSpec(memory_space=pltpu.VMEM),
                pl.BlockSpec(memory_space=pl.ANY),
            ],
            out_specs=pl.BlockSpec(memory_space=pl.ANY),
            scratch_shapes=[
                pltpu.SemaphoreType.DMA((late * m,)),
                pltpu.SemaphoreType.DMA((late * m,)),
            ],
            compiler_params=pltpu.CompilerParams(
                collective_id=1, has_side_effects=True, vmem_limit_bytes=8 * 2**20
            ),
            name="exchange_late",
        )(kept, block_sums)
        restored, block_sums = pl.pallas_call(
            lambda *refs: widen_late(n, *refs),
            out_shape=[
                jax.ShapeDtypeStruct(restored.shape, jnp.float32),
                jax.ShapeDtypeStruct(block_sums.shape, jnp.float32),
            ],
            in_specs=[
                pl.BlockSpec(memory_space=pltpu.VMEM),
                pl.BlockSpec(memory_space=pl.ANY),
                pl.BlockSpec(memory_space=pltpu.VMEM),
            ],
            out_specs=[
                pl.BlockSpec(memory_space=pl.ANY),
                pl.BlockSpec(memory_space=pl.ANY),
            ],
            scratch_shapes=[
                pltpu.VMEM((late, height, cols), jnp.float32),
                pltpu.VMEM((blocks + 8, cols), jnp.float32),
                pltpu.SemaphoreType.DMA((late,)),
                pltpu.SemaphoreType.DMA,
            ],
            input_output_aliases={1: 0},
            compiler_params=pltpu.CompilerParams(vmem_limit_bytes=20 * 2**20),
            name="widen_late",
        )(arrived, restored, block_sums)
    return (restored[None], block_sums[None])


def solution(mesh):
    n = mesh.shape["section"]
    m = mesh.shape["tensor"]
    return jax.shard_map(
        lambda saved, offsets: body(n, m, saved, offsets),
        mesh=mesh,
        in_specs=(P("section", None, "tensor", None), P("section", None)),
        out_specs=(P("section", None, None, "tensor"), P("section", None, "tensor")),
        check_vma=False,
    )
```

```python
import jax
import jax.numpy as jnp
from jax import lax
from jax.experimental import pallas as pl
from jax.experimental.pallas import tpu as pltpu
from jax.sharding import PartitionSpec as P

MESH = pl.DeviceIdType.MESH


def power_of_two(count):
    return count & (count - 1) == 0


def partner(index, step, count):
    if not power_of_two(count):
        return (index + step) % count
    other = index
    bit = 1
    while bit < count:
        if step & bit:
            other = other + bit * (1 - 2 * ((index // bit) % 2))
        bit *= 2
    return other


def late_steps(n):
    if n < 8 or not power_of_two(n):
        return []
    return list(range(3 * n // 4, n, 2))


def is_inner(s, n):
    quarter = s // (n // 4)
    return (quarter == 1) | (quarter == 2)


def is_late(s, n):
    return is_inner(s, n) & (s % 2 == 1)


def early_step(n):
    return 3 * n // 4 + 1


def send_order(n, m):
    late = late_steps(n)
    far_steps = [k for k in range(n // 2, n) if k not in late] + late
    far = [(k, e) for k in far_steps for e in range(m)]
    near = [(k, e) for k in range(n // 2 - 1, -1, -1) for e in range(m)]
    mixed = []
    for i in range(max(len(far), len(near))):
        mixed += far[i : i + 1] + near[i : i + 1]
    return mixed


def parts_of(cols):
    if cols % 1024:
        return [cols]
    return [cols // 8, cols // 8, cols // 4, cols // 2]


def signal(barrier, t, d):
    pl.semaphore_signal(barrier, inc=1, device_id=(t, d), device_id_type=MESH)


def greet_outer(barrier, n, m, first, s, x):
    half = n // 2

    def greet(j, carry):
        place = (s + j // m) % half
        t = jnp.where(place < n // 4, place, place + half)
        signal(barrier, t, (x + j % m) % m)
        return carry

    lax.fori_loop(first, half * m, greet, 0)


def greet_all(barrier, n, m, s, x):
    def greet(j, carry):
        signal(barrier, (s + j // m) % n, (x + j % m) % m)
        return carry

    lax.fori_loop(1, n * m, greet, 0)


def exchange(
    n, m, offsets, saved, arrived, kept, table, rest, out_box,
    table_sem, load_sem, send_sem, recv_sem, own_sem, part_sem, *pieces,
):
    s = lax.axis_index("section")
    x = lax.axis_index("tensor")
    rows = saved.shape[1]
    cols = saved.shape[2] // m
    parts = len(pieces)
    widths = parts_of(cols)
    starts = [sum(widths[:h]) for h in range(parts)]
    late = late_steps(n)
    staged = bool(late)
    first = early_step(n) if staged else n // 2
    barrier = pltpu.get_barrier_semaphore()
    inner = is_inner(s, n) if staged else None

    tabled = pltpu.make_async_copy(offsets, table, table_sem)
    tabled.start()
    loads = []
    for h, piece in enumerate(pieces):
        own = pl.ds(pl.multiple_of(x * cols + starts[h], widths[0]), widths[h])
        loads.append(pltpu.make_async_copy(saved.at[:, :, own], piece, load_sem.at[h]))
    for e in range(1, m):
        d = partner(x, e, m)
        those = pl.ds(pl.multiple_of(d * cols, cols), cols)
        loads.append(
            pltpu.make_async_copy(saved.at[:, :, those], rest.at[e - 1], load_sem.at[parts - 1 + e])
        )
    for load in loads:
        load.start()

    if staged:

        @pl.when(inner)
        def _():
            signal(barrier, partner(s, first, n), x)

        @pl.when(jnp.logical_not(inner))
        def _():
            greet_outer(barrier, n, m, 1, jnp.where(s < n // 4, s, s - n // 2), x)

    else:
        greet_all(barrier, n, m, s, x)

    early = [k for k in range(n) if k not in late]

    def box(k, e):
        if k in late:
            return kept.at[late.index(k) * m + e]
        return out_box.at[early.index(k) * m + e]

    def slot_of(k):
        wanted = (partner(s, k, n) - s + n) % n
        slot = jnp.int32(0)
        for j in range(n):
            slot = jnp.where(table[0, j] == wanted, jnp.int32(j), slot)
        return slot

    def fill(held, slot, to, at=0):
        width = held.shape[-1]
        step = min(width, 512)

        def move(i, carry):
            here = pl.ds(pl.multiple_of(i * step, step), step)
            there = pl.ds(pl.multiple_of(at + i * step, widths[0]), step)
            to[:, there] = held[slot, :, here]
            return carry

        lax.fori_loop(0, width // step, move, 0)

    def fill_block(k, e):
        slot = slot_of(k)
        to = box(k, e)
        if e == 0:
            for h, piece in enumerate(pieces):
                fill(piece, slot, to, starts[h])
        else:
            fill(rest.at[e - 1], slot, to)

    def send(k, e):
        dst = arrived.at[s, pl.ds(x * rows, rows), :]
        if k == 0 and e == 0:
            return pltpu.make_async_copy(box(k, e), dst, own_sem)
        return pltpu.make_async_remote_copy(
            src_ref=box(k, e),
            dst_ref=dst,
            send_sem=send_sem.at[k * m + e],
            recv_sem=recv_sem.at[k * m + e],
            device_id=(partner(s, k, n), partner(x, e, m)),
            device_id_type=MESH,
        )

    def send_part(h):
        return pltpu.make_async_remote_copy(
            src_ref=box(first, 0).at[:, pl.ds(starts[h], widths[h])],
            dst_ref=arrived.at[s, pl.ds(x * rows, rows), pl.ds(starts[h], widths[h])],
            send_sem=part_sem.at[h],
            recv_sem=part_sem.at[parts + h],
            device_id=(partner(s, first, n), x),
            device_id_type=MESH,
        )

    firsts = [send_part(h) for h in range(parts)]
    if staged:

        @pl.when(inner)
        def _():
            pl.semaphore_wait(barrier, 1)
            greet_outer(barrier, n, m, 0, 0, 0)

    tabled.wait()
    slot = slot_of(first)
    for h in range(parts):
        loads[h].wait()
        fill(pieces[h], slot, box(first, 0), starts[h])
        if h > 0:
            firsts[h].start()
        elif staged:

            @pl.when(inner)
            def _():
                firsts[0].start()

            @pl.when(jnp.logical_not(inner))
            def _():
                pl.semaphore_wait(barrier, n * m - 1)
                signal(barrier, partner(s, n // 4, n), x)
                firsts[0].start()

        else:
            pl.semaphore_wait(barrier, n * m - 1)
            firsts[0].start()
    for load in loads[parts:]:
        load.wait()

    def start(k, e):
        copy = send(k, e)
        if k in late:
            pl.when(jnp.logical_not(is_late(s, n)))(copy.start)
        else:
            copy.start()
        copies.append((k, copy))

    copies = []
    waiting = None
    for k, e in send_order(n, m):
        if k == first and e == 0:
            continue
        fill_block(k, e)
        if waiting is not None:
            if staged and not copies:

                @pl.when(inner)
                def _():
                    pl.semaphore_wait(barrier, 1)

            start(*waiting)
        waiting = (k, e)
    start(*waiting)
    for copy in firsts:
        copy.wait()
    for k, copy in copies:
        if k not in late:
            copy.wait()

    if late:

        @pl.when(jnp.logical_not(is_late(s, n)))
        def _():
            for k, copy in copies:
                if k in late:
                    copy.wait()


def exchange_late(n, m, kept, sums, arrived, send_sem, recv_sem):
    s = lax.axis_index("section")
    x = lax.axis_index("tensor")
    rows = kept.shape[1]
    late = late_steps(n)
    pairs = [(k, e) for k in late for e in range(m)]
    barrier = pltpu.get_barrier_semaphore()

    @pl.when(is_late(s, n))
    def _():
        for k, e in pairs:
            pl.semaphore_signal(
                barrier,
                inc=1,
                device_id=(partner(s, k, n), partner(x, e, m)),
                device_id_type=MESH,
            )
        pl.semaphore_wait(barrier, len(pairs))
        copies = []
        for i, (k, e) in reversed(list(enumerate(pairs))):
            copy = pltpu.make_async_remote_copy(
                src_ref=kept.at[i],
                dst_ref=arrived.at[late.index(k), pl.ds(x * rows, rows), :],
                send_sem=send_sem.at[i],
                recv_sem=recv_sem.at[i],
                device_id=(partner(s, k, n), partner(x, e, m)),
                device_id_type=MESH,
            )
            copy.start()
            copies.append(copy)
        for copy in copies:
            copy.wait()


def widen_block(arrived, i, restored, sums, at, stage, sem, eager=False):
    _, rows, cols = arrived.shape
    wide = min(cols, 512)
    for c in range(0, cols, wide):
        here = pl.ds(c, wide)
        total = None
        for r in range(0, rows, 16):
            band = pl.ds(r, min(16, rows - r))
            part = arrived[i, band, here].astype(jnp.float32)
            stage[band, here] = part
            total = part if total is None else total + part
        sums[pl.ds(at, 1), here] = jnp.sum(total, axis=0, keepdims=True)
        if eager:
            pltpu.make_async_copy(stage.at[:, here], restored.at[at, :, here], sem).start()
    if eager:
        return None
    copy = pltpu.make_async_copy(stage, restored.at[at], sem)
    copy.start()
    return copy


def widen(n, arrived, restored, sums, stage, table, stage_sem):
    s = lax.axis_index("section")
    late = late_steps(n)
    depth = stage.shape[0] - len(late)
    copies = []
    for k in range(n):
        if k in late:
            continue
        slot = len(copies) % depth
        if len(copies) >= depth:
            copies[len(copies) - depth].wait()
        i = partner(s, k, n)
        copies.append(
            widen_block(arrived, i, restored, table, i, stage.at[slot], stage_sem.at[slot])
        )
    if late:

        @pl.when(jnp.logical_not(is_late(s, n)))
        def _():
            rest = []
            for j, k in enumerate(late):
                i = partner(s, k, n)
                slot = depth + j
                rest.append(
                    widen_block(arrived, i, restored, table, i, stage.at[slot], stage_sem.at[slot])
                )
            for copy in rest:
                copy.wait()

    sums[...] = table[pl.ds(0, n), :]
    for copy in copies[-depth:]:
        copy.wait()


def widen_late(n, arrived, given, sums, restored, sums_out, stage, table, stage_sem, table_sem):
    s = lax.axis_index("section")
    late = late_steps(n)
    table[pl.ds(0, n), :] = sums[...]

    places = [partner(s, k, n) for k in late]

    @pl.when(is_late(s, n))
    def _():
        for j, i in enumerate(places):
            widen_block(
                arrived, j, restored, table, i, stage.at[j], stage_sem.at[j], eager=True
            )

    copy = pltpu.make_async_copy(table.at[pl.ds(0, n), :], sums_out, table_sem)
    copy.start()

    @pl.when(is_late(s, n))
    def _():
        for j, i in enumerate(places):
            pltpu.make_async_copy(stage.at[j], restored.at[i], stage_sem.at[j]).wait()

    copy.wait()


def body(n, m, saved, offsets):
    _, slots, rows, width = saved.shape
    cols = width // m
    late = len(late_steps(n))
    widths = parts_of(cols)
    parts = len(widths)
    arrived, kept = pl.pallas_call(
        lambda *refs: exchange(n, m, *refs),
        out_shape=[
            jax.ShapeDtypeStruct((slots, rows * m, cols), saved.dtype),
            jax.ShapeDtypeStruct((max(late * m, 1), rows, cols), saved.dtype),
        ],
        in_specs=[
            pl.BlockSpec(memory_space=pltpu.HBM),
            pl.BlockSpec(memory_space=pltpu.HBM),
        ],
        out_specs=[
            pl.BlockSpec(memory_space=pl.ANY),
            pl.BlockSpec(memory_space=pltpu.VMEM),
        ],
        scratch_shapes=[
            pltpu.SMEM(offsets.shape, offsets.dtype),
            pltpu.VMEM((max(m - 1, 1), slots, rows, cols), saved.dtype),
            pltpu.VMEM(((slots - late) * m, rows, cols), saved.dtype),
            pltpu.SemaphoreType.DMA,
            pltpu.SemaphoreType.DMA((parts + m - 1,)),
            pltpu.SemaphoreType.DMA((n * m,)),
            pltpu.SemaphoreType.DMA((n * m,)),
            pltpu.SemaphoreType.DMA,
            pltpu.SemaphoreType.DMA((2 * parts,)),
        ]
        + [pltpu.VMEM((slots, rows, width), saved.dtype) for width in widths],
        compiler_params=pltpu.CompilerParams(
            collective_id=0, has_side_effects=True, vmem_limit_bytes=20 * 2**20
        ),
        name="exchange",
    )(
        pltpu.with_memory_space_constraint(offsets, pltpu.HBM),
        pltpu.with_memory_space_constraint(saved[0], pltpu.HBM),
    )
    blocks, height = arrived.shape[:2]
    restored, block_sums = pl.pallas_call(
        lambda *refs: widen(n, *refs),
        out_shape=[
            jax.ShapeDtypeStruct(arrived.shape, jnp.float32),
            jax.ShapeDtypeStruct((blocks, cols), jnp.float32),
        ],
        in_specs=[pl.BlockSpec(memory_space=pltpu.VMEM)],
        out_specs=[
            pl.BlockSpec(memory_space=pl.ANY),
            pl.BlockSpec(memory_space=pltpu.VMEM),
        ],
        scratch_shapes=[
            pltpu.VMEM((6 + late, height, cols), jnp.float32),
            pltpu.VMEM((blocks + 8, cols), jnp.float32),
            pltpu.SemaphoreType.DMA((6 + late,)),
        ],
        compiler_params=pltpu.CompilerParams(vmem_limit_bytes=20 * 2**20),
        name="widen",
    )(arrived)
    if late:
        arrived = pl.pallas_call(
            lambda *refs: exchange_late(n, m, *refs),
            out_shape=jax.ShapeDtypeStruct((late, rows * m, cols), saved.dtype),
            in_specs=[
                pl.BlockSpec(memory_space=pltpu.VMEM),
                pl.BlockSpec(memory_space=pl.ANY),
            ],
            out_specs=pl.BlockSpec(memory_space=pl.ANY),
            scratch_shapes=[
                pltpu.SemaphoreType.DMA((late * m,)),
                pltpu.SemaphoreType.DMA((late * m,)),
            ],
            compiler_params=pltpu.CompilerParams(
                collective_id=1, has_side_effects=True, vmem_limit_bytes=8 * 2**20
            ),
            name="exchange_late",
        )(kept, block_sums)
        restored, block_sums = pl.pallas_call(
            lambda *refs: widen_late(n, *refs),
            out_shape=[
                jax.ShapeDtypeStruct(restored.shape, jnp.float32),
                jax.ShapeDtypeStruct(block_sums.shape, jnp.float32),
            ],
            in_specs=[
                pl.BlockSpec(memory_space=pltpu.VMEM),
                pl.BlockSpec(memory_space=pl.ANY),
                pl.BlockSpec(memory_space=pltpu.VMEM),
            ],
            out_specs=[
                pl.BlockSpec(memory_space=pl.ANY),
                pl.BlockSpec(memory_space=pl.ANY),
            ],
            scratch_shapes=[
                pltpu.VMEM((late, height, cols), jnp.float32),
                pltpu.VMEM((blocks + 8, cols), jnp.float32),
                pltpu.SemaphoreType.DMA((late,)),
                pltpu.SemaphoreType.DMA,
            ],
            input_output_aliases={1: 0},
            compiler_params=pltpu.CompilerParams(vmem_limit_bytes=20 * 2**20),
            name="widen_late",
        )(arrived, restored, block_sums)
    return (restored[None], block_sums[None])


def solution(mesh):
    n = mesh.shape["section"]
    m = mesh.shape["tensor"]
    return jax.shard_map(
        lambda saved, offsets: body(n, m, saved, offsets),
        mesh=mesh,
        in_specs=(P("section", None, "tensor", None), P("section", None)),
        out_specs=(P("section", None, None, "tensor"), P("section", None, "tensor")),
        check_vma=False,
    )
```

```python
import jax
import jax.numpy as jnp
from jax import lax
from jax.experimental import pallas as pl
from jax.experimental.pallas import tpu as pltpu
from jax.sharding import PartitionSpec as P

MESH = pl.DeviceIdType.MESH


def power_of_two(count):
    return count & (count - 1) == 0


def partner(index, step, count):
    if not power_of_two(count):
        return (index + step) % count
    other = index
    bit = 1
    while bit < count:
        if step & bit:
            other = other + bit * (1 - 2 * ((index // bit) % 2))
        bit *= 2
    return other


def late_steps(n):
    if n < 8 or not power_of_two(n):
        return []
    return list(range(3 * n // 4, n, 2))


def is_inner(s, n):
    quarter = s // (n // 4)
    return (quarter == 1) | (quarter == 2)


def is_late(s, n):
    return is_inner(s, n) & (s % 2 == 1)


def early_step(n):
    return 3 * n // 4 + 1


def send_order(n, m):
    late = late_steps(n)
    far_steps = [k for k in range(n // 2, n) if k not in late] + late
    far = [(k, e) for k in far_steps for e in range(m)]
    near = [(k, e) for k in range(n // 2 - 1, -1, -1) for e in range(m)]
    mixed = []
    for i in range(max(len(far), len(near))):
        mixed += far[i : i + 1] + near[i : i + 1]
    return mixed


def parts_of(cols):
    if cols % 1024:
        return [cols]
    return [cols // 8, cols // 8, cols // 4, cols // 2]


def signal(barrier, t, d):
    pl.semaphore_signal(barrier, inc=1, device_id=(t, d), device_id_type=MESH)


def greet_outer(barrier, n, m, first, s, x):
    half = n // 2

    def greet(j, carry):
        place = (s + j // m) % half
        t = jnp.where(place < n // 4, place, place + half)
        signal(barrier, t, (x + j % m) % m)
        return carry

    lax.fori_loop(first, half * m, greet, 0)


def greet_all(barrier, n, m, s, x):
    def greet(j, carry):
        signal(barrier, (s + j // m) % n, (x + j % m) % m)
        return carry

    lax.fori_loop(1, n * m, greet, 0)


def exchange(
    n, m, offsets, saved, arrived, kept, table, rest, out_box,
    table_sem, load_sem, send_sem, recv_sem, own_sem, part_sem, *pieces,
):
    s = lax.axis_index("section")
    x = lax.axis_index("tensor")
    rows = saved.shape[1]
    cols = saved.shape[2] // m
    parts = len(pieces)
    widths = parts_of(cols)
    starts = [sum(widths[:h]) for h in range(parts)]
    late = late_steps(n)
    staged = bool(late)
    first = early_step(n) if staged else n // 2
    barrier = pltpu.get_barrier_semaphore()
    inner = is_inner(s, n) if staged else None

    tabled = pltpu.make_async_copy(offsets, table, table_sem)
    tabled.start()
    loads = []
    for h, piece in enumerate(pieces):
        own = pl.ds(pl.multiple_of(x * cols + starts[h], widths[0]), widths[h])
        loads.append(pltpu.make_async_copy(saved.at[:, :, own], piece, load_sem.at[h]))
    for e in range(1, m):
        d = partner(x, e, m)
        those = pl.ds(pl.multiple_of(d * cols, cols), cols)
        loads.append(
            pltpu.make_async_copy(saved.at[:, :, those], rest.at[e - 1], load_sem.at[parts - 1 + e])
        )
    for load in loads:
        load.start()

    if staged:

        @pl.when(inner)
        def _():
            signal(barrier, partner(s, first, n), x)

        @pl.when(jnp.logical_not(inner))
        def _():
            greet_outer(barrier, n, m, 1, jnp.where(s < n // 4, s, s - n // 2), x)

    else:
        greet_all(barrier, n, m, s, x)

    early = [k for k in range(n) if k not in late]

    def box(k, e):
        if k in late:
            return kept.at[late.index(k) * m + e]
        return out_box.at[early.index(k) * m + e]

    def slot_of(k):
        wanted = (partner(s, k, n) - s + n) % n
        slot = jnp.int32(0)
        for j in range(n):
            slot = jnp.where(table[0, j] == wanted, jnp.int32(j), slot)
        return slot

    def fill(held, slot, to, at=0):
        width = held.shape[-1]
        step = min(width, 512)

        def move(i, carry):
            here = pl.ds(pl.multiple_of(i * step, step), step)
            there = pl.ds(pl.multiple_of(at + i * step, widths[0]), step)
            to[:, there] = held[slot, :, here]
            return carry

        lax.fori_loop(0, width // step, move, 0)

    def fill_block(k, e):
        slot = slot_of(k)
        to = box(k, e)
        if e == 0:
            for h, piece in enumerate(pieces):
                fill(piece, slot, to, starts[h])
        else:
            fill(rest.at[e - 1], slot, to)

    def send(k, e):
        dst = arrived.at[s, pl.ds(x * rows, rows), :]
        if k == 0 and e == 0:
            return pltpu.make_async_copy(box(k, e), dst, own_sem)
        return pltpu.make_async_remote_copy(
            src_ref=box(k, e),
            dst_ref=dst,
            send_sem=send_sem.at[k * m + e],
            recv_sem=recv_sem.at[k * m + e],
            device_id=(partner(s, k, n), partner(x, e, m)),
            device_id_type=MESH,
        )

    def send_part(h):
        return pltpu.make_async_remote_copy(
            src_ref=box(first, 0).at[:, pl.ds(starts[h], widths[h])],
            dst_ref=arrived.at[s, pl.ds(x * rows, rows), pl.ds(starts[h], widths[h])],
            send_sem=part_sem.at[h],
            recv_sem=part_sem.at[parts + h],
            device_id=(partner(s, first, n), x),
            device_id_type=MESH,
        )

    firsts = [send_part(h) for h in range(parts)]
    if staged:

        @pl.when(inner)
        def _():
            pl.semaphore_wait(barrier, 1)
            greet_outer(barrier, n, m, 0, 0, 0)

    tabled.wait()
    slot = slot_of(first)
    for h in range(parts):
        loads[h].wait()
        fill(pieces[h], slot, box(first, 0), starts[h])
        if h > 0:
            firsts[h].start()
        elif staged:

            @pl.when(inner)
            def _():
                firsts[0].start()

            @pl.when(jnp.logical_not(inner))
            def _():
                pl.semaphore_wait(barrier, n * m - 1)
                signal(barrier, partner(s, n // 4, n), x)
                firsts[0].start()

        else:
            pl.semaphore_wait(barrier, n * m - 1)
            firsts[0].start()
    for load in loads[parts:]:
        load.wait()

    def start(k, e):
        copy = send(k, e)
        if k in late:
            pl.when(jnp.logical_not(is_late(s, n)))(copy.start)
        else:
            copy.start()
        copies.append((k, copy))

    copies = []
    waiting = None
    for k, e in send_order(n, m):
        if k == first and e == 0:
            continue
        fill_block(k, e)
        if waiting is not None:
            if staged and not copies:

                @pl.when(inner)
                def _():
                    pl.semaphore_wait(barrier, 1)

            start(*waiting)
        waiting = (k, e)
    start(*waiting)
    for copy in firsts:
        copy.wait()
    for k, copy in copies:
        if k not in late:
            copy.wait()

    if late:

        @pl.when(jnp.logical_not(is_late(s, n)))
        def _():
            for k, copy in copies:
                if k in late:
                    copy.wait()


def exchange_late(n, m, kept, sums, arrived, send_sem, recv_sem):
    s = lax.axis_index("section")
    x = lax.axis_index("tensor")
    rows = kept.shape[1]
    late = late_steps(n)
    pairs = [(k, e) for k in late for e in range(m)]
    barrier = pltpu.get_barrier_semaphore()

    @pl.when(is_late(s, n))
    def _():
        for k, e in pairs:
            pl.semaphore_signal(
                barrier,
                inc=1,
                device_id=(partner(s, k, n), partner(x, e, m)),
                device_id_type=MESH,
            )
        pl.semaphore_wait(barrier, len(pairs))
        copies = []
        for i, (k, e) in reversed(list(enumerate(pairs))):
            copy = pltpu.make_async_remote_copy(
                src_ref=kept.at[i],
                dst_ref=arrived.at[late.index(k), pl.ds(x * rows, rows), :],
                send_sem=send_sem.at[i],
                recv_sem=recv_sem.at[i],
                device_id=(partner(s, k, n), partner(x, e, m)),
                device_id_type=MESH,
            )
            copy.start()
            copies.append(copy)
        for copy in copies:
            copy.wait()


def widen_block(arrived, i, restored, sums, at, stage, sem, row=None, eager=False):
    _, rows, cols = arrived.shape
    row = at if row is None else row
    wide = min(cols, 512)
    for c in range(0, cols, wide):
        here = pl.ds(c, wide)
        total = None
        for r in range(0, rows, 16):
            band = pl.ds(r, min(16, rows - r))
            part = arrived[i, band, here].astype(jnp.float32)
            stage[band, here] = part
            total = part if total is None else total + part
        sums[pl.ds(row, 1), here] = jnp.sum(total, axis=0, keepdims=True)
        if eager:
            pltpu.make_async_copy(stage.at[:, here], restored.at[at, :, here], sem).start()
    if eager:
        return None
    copy = pltpu.make_async_copy(stage, restored.at[at], sem)
    copy.start()
    return copy


def widen(n, arrived, restored, sums, stage, table, stage_sem):
    s = lax.axis_index("section")
    late = late_steps(n)
    depth = stage.shape[0] - len(late)
    copies = []
    for k in range(n):
        if k in late:
            continue
        slot = len(copies) % depth
        if len(copies) >= depth:
            copies[len(copies) - depth].wait()
        i = partner(s, k, n)
        copies.append(
            widen_block(arrived, i, restored, table, i, stage.at[slot], stage_sem.at[slot])
        )
    if late:

        @pl.when(jnp.logical_not(is_late(s, n)))
        def _():
            rest = []
            for j, k in enumerate(late):
                i = partner(s, k, n)
                slot = depth + j
                rest.append(
                    widen_block(arrived, i, restored, table, i, stage.at[slot], stage_sem.at[slot])
                )
            for copy in rest:
                copy.wait()

    sums[...] = table[pl.ds(0, n), :]
    for copy in copies[-depth:]:
        copy.wait()


def widen_late(n, arrived, given, sums, restored, sums_out, stage, fresh, table, stage_sem, table_sem):
    s = lax.axis_index("section")
    late = late_steps(n)
    places = [partner(s, k, n) for k in late]

    @pl.when(is_late(s, n))
    def _():
        for j, i in enumerate(places):
            widen_block(
                arrived, j, restored, fresh, i, stage.at[j], stage_sem.at[j], row=j, eager=True
            )

    table[pl.ds(0, n), :] = sums[...]

    @pl.when(is_late(s, n))
    def _():
        for j, i in enumerate(places):
            table[pl.ds(i, 1), :] = fresh[pl.ds(j, 1), :]

    copy = pltpu.make_async_copy(table.at[pl.ds(0, n), :], sums_out, table_sem)
    copy.start()

    @pl.when(is_late(s, n))
    def _():
        for j, i in enumerate(places):
            pltpu.make_async_copy(stage.at[j], restored.at[i], stage_sem.at[j]).wait()

    copy.wait()


def body(n, m, saved, offsets):
    _, slots, rows, width = saved.shape
    cols = width // m
    late = len(late_steps(n))
    widths = parts_of(cols)
    parts = len(widths)
    arrived, kept = pl.pallas_call(
        lambda *refs: exchange(n, m, *refs),
        out_shape=[
            jax.ShapeDtypeStruct((slots, rows * m, cols), saved.dtype),
            jax.ShapeDtypeStruct((max(late * m, 1), rows, cols), saved.dtype),
        ],
        in_specs=[
            pl.BlockSpec(memory_space=pltpu.HBM),
            pl.BlockSpec(memory_space=pltpu.HBM),
        ],
        out_specs=[
            pl.BlockSpec(memory_space=pl.ANY),
            pl.BlockSpec(memory_space=pltpu.VMEM),
        ],
        scratch_shapes=[
            pltpu.SMEM(offsets.shape, offsets.dtype),
            pltpu.VMEM((max(m - 1, 1), slots, rows, cols), saved.dtype),
            pltpu.VMEM(((slots - late) * m, rows, cols), saved.dtype),
            pltpu.SemaphoreType.DMA,
            pltpu.SemaphoreType.DMA((parts + m - 1,)),
            pltpu.SemaphoreType.DMA((n * m,)),
            pltpu.SemaphoreType.DMA((n * m,)),
            pltpu.SemaphoreType.DMA,
            pltpu.SemaphoreType.DMA((2 * parts,)),
        ]
        + [pltpu.VMEM((slots, rows, width), saved.dtype) for width in widths],
        compiler_params=pltpu.CompilerParams(
            collective_id=0, has_side_effects=True, vmem_limit_bytes=20 * 2**20
        ),
        name="exchange",
    )(
        pltpu.with_memory_space_constraint(offsets, pltpu.HBM),
        pltpu.with_memory_space_constraint(saved[0], pltpu.HBM),
    )
    blocks, height = arrived.shape[:2]
    restored, block_sums = pl.pallas_call(
        lambda *refs: widen(n, *refs),
        out_shape=[
            jax.ShapeDtypeStruct(arrived.shape, jnp.float32),
            jax.ShapeDtypeStruct((blocks, cols), jnp.float32),
        ],
        in_specs=[pl.BlockSpec(memory_space=pltpu.VMEM)],
        out_specs=[
            pl.BlockSpec(memory_space=pl.ANY),
            pl.BlockSpec(memory_space=pltpu.VMEM),
        ],
        scratch_shapes=[
            pltpu.VMEM((6 + late, height, cols), jnp.float32),
            pltpu.VMEM((blocks + 8, cols), jnp.float32),
            pltpu.SemaphoreType.DMA((6 + late,)),
        ],
        compiler_params=pltpu.CompilerParams(vmem_limit_bytes=20 * 2**20),
        name="widen",
    )(arrived)
    if late:
        arrived = pl.pallas_call(
            lambda *refs: exchange_late(n, m, *refs),
            out_shape=jax.ShapeDtypeStruct((late, rows * m, cols), saved.dtype),
            in_specs=[
                pl.BlockSpec(memory_space=pltpu.VMEM),
                pl.BlockSpec(memory_space=pl.ANY),
            ],
            out_specs=pl.BlockSpec(memory_space=pl.ANY),
            scratch_shapes=[
                pltpu.SemaphoreType.DMA((late * m,)),
                pltpu.SemaphoreType.DMA((late * m,)),
            ],
            compiler_params=pltpu.CompilerParams(
                collective_id=1, has_side_effects=True, vmem_limit_bytes=8 * 2**20
            ),
            name="exchange_late",
        )(kept, block_sums)
        restored, block_sums = pl.pallas_call(
            lambda *refs: widen_late(n, *refs),
            out_shape=[
                jax.ShapeDtypeStruct(restored.shape, jnp.float32),
                jax.ShapeDtypeStruct(block_sums.shape, jnp.float32),
            ],
            in_specs=[
                pl.BlockSpec(memory_space=pltpu.VMEM),
                pl.BlockSpec(memory_space=pl.ANY),
                pl.BlockSpec(memory_space=pltpu.VMEM),
            ],
            out_specs=[
                pl.BlockSpec(memory_space=pl.ANY),
                pl.BlockSpec(memory_space=pl.ANY),
            ],
            scratch_shapes=[
                pltpu.VMEM((late, height, cols), jnp.float32),
                pltpu.VMEM((late + 8, cols), jnp.float32),
                pltpu.VMEM((blocks + 8, cols), jnp.float32),
                pltpu.SemaphoreType.DMA((late,)),
                pltpu.SemaphoreType.DMA,
            ],
            input_output_aliases={1: 0},
            compiler_params=pltpu.CompilerParams(vmem_limit_bytes=20 * 2**20),
            name="widen_late",
        )(arrived, restored, block_sums)
    return (restored[None], block_sums[None])


def solution(mesh):
    n = mesh.shape["section"]
    m = mesh.shape["tensor"]
    return jax.shard_map(
        lambda saved, offsets: body(n, m, saved, offsets),
        mesh=mesh,
        in_specs=(P("section", None, "tensor", None), P("section", None)),
        out_specs=(P("section", None, None, "tensor"), P("section", None, "tensor")),
        check_vma=False,
    )
```
